32 devices in a mesh: row: 8 (over y, x, core), col: 4 (over z).
Axes of the slice: x: 2, y: 2, z: 4, core: 2. Of those that a mesh axis runs over, the one named last changes fastest.
Arguments:
- choi: float32 [4, 2048, 1024], P(None, 'row', 'col'), may hold values from -0.5 to 8, as said below
Outputs:
- factored: float32 [4, 2048, 1024], P(None, 'row', 'col')
The draws below stay inside these ranges and needn't reach their ends.
Inputs may be any that keep to these rules, and one draw needn't show every extreme that they name: `choi`: the leading 1024 x 1024 block of the matrix is symmetric with a positive diagonal, and its leading 2 * 256 square is positive definite.
All inputs are finite; a program needn't handle non-finite values.
Results may differ from the reference program's by a relative error of at most 0.0001.
Values sent between devices are 32-bit elements; how exact they have to be, the bound alone decides.
A program may use at most 64 MiB of HBM per device.

```python
import math
import jax
import jax.numpy as jnp
from jax import lax

TILE = 256
RT_DEV = 4
PANELS = 2
ORDER = 8192
COLS = 1024
N_ROW = 8


off_spread = 0.04


def draw_choi(key, part):
    first = jax.random.fold_in(key, 11)
    second = jax.random.fold_in(key, 23)
    noise_draw = jax.random.normal(first, (ORDER, COLS), jnp.float32) * off_spread
    diag_draw = jax.random.uniform(second, (COLS,), jnp.float32, 4.5, 8.0)
    upper_part = noise_draw[:COLS]
    symmetric = (upper_part + upper_part.T) * math.sqrt(0.5)
    ident_mask = jnp.arange(COLS)[:, None] == jnp.arange(COLS)[None, :]
    symmetric = jnp.where(ident_mask, diag_draw[:, None], symmetric)
    whole_matrix = jnp.concatenate([symmetric, noise_draw[COLS:]], axis=0)
    return whole_matrix.reshape(RT_DEV, ORDER // RT_DEV, COLS)


def setup_inputs(seed: int = 0) -> dict:
    splits = jax.random.split(jax.random.key(seed), 2)
    return {
        "choi": draw_choi(jax.random.fold_in(splits[1], 71), 0),
    }


def reference(choi):
    matrix = choi.reshape(RT_DEV * N_ROW * TILE, COLS)
    identity = jnp.eye(TILE, dtype=matrix.dtype)
    for step in range(PANELS):
        start = step * TILE
        finish = start + TILE
        factor = jnp.linalg.cholesky(matrix[start:finish, start:finish])
        inverse = jax.scipy.linalg.solve_triangular(factor, identity, lower=True)
        beneath = jnp.dot(matrix[finish:, start:finish], inverse.T, precision=lax.Precision.HIGHEST)
        column = jnp.concatenate([jnp.zeros((start, TILE), matrix.dtype), factor, beneath], axis=0)
        matrix = matrix.at[:, start:finish].set(column)
        change = jnp.dot(beneath, beneath[:COLS - finish].T, precision=lax.Precision.HIGHEST)
        matrix = matrix.at[finish:, finish:].add(-change)
    matrix = matrix.at[:PANELS * TILE, PANELS * TILE:].set(0.0)
    return matrix.reshape(RT_DEV, N_ROW * TILE, COLS)
```

```python
import functools

import jax
import jax.numpy as jnp
from jax import lax
from jax.experimental import pallas as pl
from jax.experimental.pallas import tpu as pltpu
from jax.sharding import PartitionSpec as P

MESH = pl.DeviceIdType.MESH
HIGHEST = lax.Precision.HIGHEST
F32 = jnp.float32

PIECES = 4
ITEMS = (
    (0, 1, 0, 0, 0, 0, 2, 4, True),
    (0, 1, 0, 0, 0, 2, 2, 4, True),
    (0, 1, 0, 0, 0, 4, 2, 8, False),
    (0, 1, 0, 0, 0, 6, 2, 8, False),
    (1, 1, 1, 0, 1, 0, 2, 8, False),
    (1, 1, 1, 0, 1, 2, 2, 8, False),
    (1, 1, 1, 0, 1, 4, 2, 8, False),
    (1, 1, 1, 0, 1, 6, 2, 8, False),
    (2, 1, 1, 1, 1, 0, 4, 4, False),
    (2, 1, 1, 1, 1, 4, 2, 8, False),
    (2, 1, 1, 1, 1, 6, 2, 8, False),
    (3, 0, 0, None, 2, 0, 2, 8, False),
    (3, 0, 0, None, 2, 2, 2, 8, False),
    (3, 0, 0, None, 2, 4, 2, 8, False),
    (3, 0, 0, None, 2, 6, 2, 8, False),
    (4, 1, 1, None, 2, 0, 2, 8, False),
    (4, 1, 1, None, 2, 2, 2, 8, False),
    (4, 1, 1, None, 2, 4, 2, 8, False),
    (4, 1, 1, None, 2, 6, 2, 8, False),
)
FIRST, REST, BELOW, CORNER, TOP, NEXT = (
    (0, 1), (2, 3), (4, 5, 6, 7), (8, 9, 10), (11, 12, 13, 14), (15, 16, 17, 18),
)

TICKS = {
    "start": (4, 0),
    0: ((1, 0), (1, 1), (1, 1), (1, 1), (2, 2)),
    1: ((1, 1), (1, 1), (1, 1), (1, 1), (2, 2)),
    2: ((1, 1), (1, 1), (1, 1), (1, 1), (2, 1)),
    3: ((1, 1), (1, 1), (1, 1), (1, 1), (2, 2)),
}


def dot(a, b, ca=1, cb=0, precision=HIGHEST):
    return lax.dot_general(
        a, b, (((ca,), (cb,)), ((), ())), precision=precision, preferred_element_type=F32
    )


def split(x):
    high = x.astype(jnp.bfloat16)
    return high, (x - high.astype(F32)).astype(jnp.bfloat16)


def dot3(a, b):
    (ah, al), (bh, bl) = a, b

    def one(x, y):
        return jnp.dot(x, y, preferred_element_type=F32)

    return one(al, bh) + one(ah, bl) + one(ah, bh)


def pivot_rows(rows, lane, sub, first):
    n = rows.shape[1]
    wide = [jnp.broadcast_to(rows[j : j + 1, :], (8, n)) for j in range(8)]
    columns = [
        jnp.sum(jnp.where(lane == first + j, rows, 0.0), axis=1, keepdims=True) for j in range(8)
    ]
    columns = [jnp.broadcast_to(c, (8, n)) for c in columns]
    entry = [
        [jnp.broadcast_to(columns[j][i : i + 1, :], (8, n)) if j <= i else None for j in range(8)]
        for i in range(8)
    ]
    final = jnp.zeros((8, n), F32)
    for j in range(8):
        here = lane == first + j
        pivot = entry[j][j]
        inverse = 1.0 / pivot
        base = jnp.where(here, 1.0, wide[j])
        final = jnp.where(sub == j, base * lax.rsqrt(pivot), final)
        for i in range(j + 1, 8):
            scale = entry[i][j] * inverse
            wide[i] = jnp.where(here, 0.0, wide[i]) - scale * base
            for t in range(j + 1, i + 1):
                entry[i][t] = entry[i][t] - scale * entry[t][j]
    return final


def invert_factor(z_ref, between):
    n = z_ref.shape[0]
    lane = lax.broadcasted_iota(jnp.int32, (8, n), 1)
    sub = lax.broadcasted_iota(jnp.int32, (8, n), 0)
    all_lane = lax.broadcasted_iota(jnp.int32, (n, n), 1)
    all_row = lax.broadcasted_iota(jnp.int32, (n, n), 0)

    def group(g, carry):
        first = pl.multiple_of(8 * g, 8)
        final = pivot_rows(z_ref[pl.ds(first, 8), :], lane, sub, first)
        right = jnp.where((lane < first + 8) & (lane > first + sub), 0.0, final)
        left = jnp.where(lane >= first + 8, final, 0.0)
        change = dot(left, right, 0, 0)
        mine = (all_lane >= first) & (all_lane < first + 8) & (all_row >= first + 8)
        z_ref[...] = jnp.where(mine, 0.0, z_ref[...]) - change
        z_ref[pl.ds(first, 8), :] = right
        return carry

    quarter = n // 32
    for part in range(4):
        lax.fori_loop(part * quarter, (part + 1) * quarter, group, 0)
        between(part)
    z_ref[...] = jnp.where(all_lane <= all_row, z_ref[...], 0.0)


def kernel(
    rows, cols, a_ref, o_ref, tiles, slab, blocks, work, inverse, rhs, keep, w_high, w_low,
    tile_send, tile_recv, slab_send, slab_recv,
):
    slots, size, _ = a_ref.shape
    half = size // 2
    eighth = size // 8
    part_rows = size // PIECES
    r = lax.axis_index("row")
    c = lax.axis_index("col")
    bits = [k for k in range(rows.bit_length()) if (1 << k) < rows][::-1]
    leaders = list(range(2, rows, 2))
    far_leaders = [q for q in leaders if q & (q - 1)]

    def across(k):
        return r + (1 << k) * (1 - 2 * ((r // (1 << k)) % 2))

    barrier = pltpu.get_barrier_semaphore()
    peers = []

    def greet(when, device, count=1):
        def signal():
            pl.semaphore_signal(barrier, inc=1, device_id=device, device_id_type=MESH)

        if when is None:
            signal()
            peers.append(1)
        else:
            pl.when(when)(signal)
            peers.append(jnp.where(when, 1, 0))

    for k in bits:
        greet(None, (across(k), c))
    greet(c > 0, (r, c - 1))
    greet(c < cols - 1, (r, c + 1))
    for q in far_leaders:
        greet(r == 1, (q + 1, c))
        greet(r == q + 1, (1, c))
    pl.semaphore_wait(barrier, functools.reduce(lambda x, y: x + y, peers))

    def node(root):
        return r if root == 0 else r + 1 - 2 * (r % 2)

    def item_copy(item, source, way, device):
        tile, _, _, _, _, row0, height, width, _ = ITEMS[item]
        span = (pl.ds(row0 * eighth, height * eighth), pl.ds(0, width * eighth))
        return pltpu.make_async_remote_copy(
            src_ref=source.at[span],
            dst_ref=tiles.at[(tile,) + span],
            send_sem=tile_send.at[tile, way],
            recv_sem=tile_recv.at[item],
            device_id=device,
            device_id_type=MESH,
        )

    def owns(item):
        _, _, owner_row, owner_col, first_col = ITEMS[item][:5]
        return (r == owner_row) & ((c >= first_col) if owner_col is None else (c == owner_col))

    def routes(items, visit):
        for item in items:
            tile, root, owner_row, owner_col, first_col = ITEMS[item][:5]
            straight = ITEMS[item][8]
            q = node(root)
            if owner_row != root:
                visit(owns(item), 0, item)
            if owner_col is not None:
                visit((r == root) & (c >= owner_col) & (c < cols - 1), 1, item)
            if straight:
                for n in range(len(leaders)):
                    visit((c >= first_col) & (q == 0), 2 + len(bits) + n, item)
            for n, k in enumerate(bits):
                if straight and k > 0:
                    continue
                sends = (c >= first_col) & (q % (1 << (k + 1)) == 0)
                if k == 0 and owner_row != root:
                    sends = sends & ((q != 0) | (c != owner_col))
                visit(sends, 2 + n, item)

    def target(item, way):
        root = ITEMS[item][1]
        if way == 0:
            return (root, c)
        if way == 1:
            return (root, c + 1)
        if way < 2 + len(bits):
            return (across(bits[way - 2]), c)
        return (leaders[way - 2 - len(bits)] + root, c)

    def send(item, source, ways):
        def visit(when, way, item):
            if way in ways:
                pl.when(when)(lambda: item_copy(item, source, way, target(item, way)).start())

        routes((item,), visit)

    def depth_of(root):
        q = node(root)
        return sum((q // (1 << k)) % 2 for k in bits)

    onward = range(1, 2 + len(bits) + len(leaders))

    def launch(items):
        for item in items:
            ways = onward if ITEMS[item][1] == ITEMS[item][2] else (0,)
            pl.when(owns(item))(lambda item=item, ways=ways: send(item, a_ref.at[0], ways))

    def collect(items, low, high=99, which=True):
        for item in items:
            tile, root, _, _, first_col = ITEMS[item][:5]
            depth = depth_of(root)

            @pl.when(
                which
                & (c >= first_col)
                & jnp.logical_not(owns(item))
                & (depth >= low)
                & (depth <= high)
            )
            def _(item=item, tile=tile):
                item_copy(item, tiles.at[tile], 0, (r, c)).wait_recv()
                send(item, tiles.at[tile], onward)

    def slab_copy(which, s, p, source):
        span = pl.ds(p * part_rows, part_rows)
        return pltpu.make_async_remote_copy(
            src_ref=source.at[s, span],
            dst_ref=slab.at[which, s, span],
            send_sem=slab_send.at[which],
            recv_sem=slab_recv.at[which, s, p],
            device_id=(r, c + 1),
            device_id_type=MESH,
        )

    def own_slab(which, slots_from):
        for s in range(slots_from, slots):
            for p in range(PIECES):
                slab_copy(which, s, p, a_ref).start()

    launch(FIRST + REST)
    pl.when((c == 0) & (r >= 2))(lambda: own_slab(0, 0))
    if cols > 2:
        pl.when((c == 1) & (r >= 2))(lambda: own_slab(1, 0))

    for items in (FIRST, BELOW, CORNER, TOP, NEXT):

        @pl.when(owns(items[0]))
        def _(t=ITEMS[items[0]][0]):
            tiles[t] = a_ref[0]

    def land(which, s, p):
        slab_copy(which, s, p, slab.at[which]).wait_recv()

    def pass_on(which, s, p):
        land(which, s, p)
        slab_copy(which, s, p, slab.at[which]).start()

    def orders(first):
        return [(which, s, p) for which in (1, 0) for s in range(first, slots) for p in range(PIECES)]

    queues = {False: orders(0), True: orders(1)}
    done = {False: 0, True: 0}

    def serve_one(late):
        if done[late] >= len(queues[late]):
            return
        which, s, p = queues[late][done[late]]
        count = len(queues[late]) // 2
        mine = (r < 2) if late else (r >= 2)
        if done[late] < count and cols > 2:
            pl.when(mine & (c == 1))(lambda: pass_on(0, s, p))
        elif done[late] < count:
            pl.when(mine & (c == 1))(lambda: land(0, s, p))
        if cols > 3:
            pl.when(mine & (c >= 2) & (c < cols - 1))(lambda: pass_on(which, s, p))
        done[late] += 1

    def serve(main, late):
        for _ in range(main):
            serve_one(False)
        for _ in range(late):
            serve_one(True)

    def ensure(which, s, p):
        while queues[False].index((which, s, p)) >= done[False]:
            serve_one(False)
        if s >= 1:
            while queues[True].index((which, s, p)) >= done[True]:
                serve_one(True)

    collect(FIRST, 0)
    collect(REST, 0, 0)
    launch(BELOW)
    pl.when((c == 0) & (r == 1))(lambda: own_slab(0, 1))
    launch(CORNER)
    serve(*TICKS["start"])

    def between(k, part):
        if k == 0 and part == 0:
            collect(BELOW + CORNER, 0, 0, c == 1)
            if cols > 2:
                pl.when((c == 1) & (r < 2))(lambda: own_slab(1, 1))
        if k == 0 and part == 1:
            collect(REST, 1, 1)
            collect(BELOW + CORNER, 0, 0, c == 2)
        if k == 0 and part == 2:
            pl.when((c == 0) & (r == 0))(lambda: own_slab(0, 1))
            collect(REST, 2, 2)
            collect(BELOW + CORNER, 0, 0, c >= 3)
        if k == 0 and part == 3:
            collect(REST, 3)
            collect(BELOW[:2], 1, 1)
        if k == 1 and part == 0:
            collect(BELOW[2:], 1, 1)
            launch(TOP)
        if k == 1 and part == 1:
            collect(CORNER, 1, 1)
            collect(BELOW[:2], 2, 2)
        if k == 1 and part == 2:
            collect(BELOW[2:], 2, 2)
            launch(NEXT)
        if k == 1 and part == 3:
            collect(CORNER, 2, 2)
            collect(BELOW + CORNER, 3)
        if k == 2 and part == 0:
            collect(TOP + NEXT, 1, 1)
        if k == 2 and part == 2:
            collect(TOP + NEXT, 2, 2)
        if k == 2 and part == 3:
            collect(TOP + NEXT, 3)
        serve(*TICKS[k][part])

    low, high = slice(0, half), slice(half, size)

    def factor(k):
        invert_factor(work, lambda part: between(k, part))

    def halfway(n):
        m = work[...]
        inverse[n, low, low] = m
        inverse[n, low, high] = jnp.zeros((half, half), F32)
        scaled = dot(blocks[1], m, 1, 1)
        blocks[0] = dot(scaled, m)
        work[...] = blocks[2] - dot(scaled, scaled, 1, 1)

    def whole(n):
        m = work[...]
        inverse[n, high, low] = -dot(m, blocks[0])
        inverse[n, high, high] = m

    work[...] = tiles[0, low, low]
    factor(0)
    serve(*TICKS[0][4])
    blocks[1] = tiles[0, high, low]
    blocks[2] = tiles[0, high, high]
    halfway(0)
    factor(1)
    whole(0)
    serve(*TICKS[1][4])

    @pl.when(c >= 1)
    def _():
        beneath = dot(tiles[1], inverse[0], 1, 1)
        keep[0] = beneath
        corner = tiles[2] - dot(beneath, beneath, 1, 1)
        work[...] = corner[low, low]
        blocks[1] = corner[high, low]
        blocks[2] = corner[high, high]
        keep[1] = dot(beneath, inverse[0])

    lower = lax.broadcasted_iota(jnp.int32, (size, size), 0) >= lax.broadcasted_iota(
        jnp.int32, (size, size), 1
    )

    @pl.when(c == 0)
    def _():
        for s in range(slots):
            o_ref[s] = dot(a_ref[s], inverse[0], 1, 1)

        @pl.when(r == 0)
        def _():
            o_ref[0] = jnp.where(lower, o_ref[0], 0.0)

    @pl.when(c >= 1)
    def _():
        factor(2)
        serve(*TICKS[2][4])

        @pl.when(c >= 2)
        def _():
            y = dot(inverse[0], tiles[3])
            rhs[1] = tiles[4] - dot(keep[0], y)
            rhs[0] = dot(inverse[0], y, 0, 0)

        halfway(1)
        factor(3)
        whole(1)

    serve(*TICKS[3][4])
    for s in range(slots):
        for p in range(PIECES):
            ensure(1, s, p)

    @pl.when(c == 1)
    def _():
        rhs[0] = dot(inverse[1], keep[1])
        for s in range(slots):
            o_ref[s] = dot(a_ref[s], inverse[1], 1, 1)

        @pl.when(r == 1)
        def _():
            o_ref[0] = jnp.where(lower, o_ref[0] - dot(tiles[1], rhs[0], 1, 1), 0.0)

        @pl.when(r == 0)
        def _():
            o_ref[0] = jnp.zeros((size, size), F32)

        @pl.when(r >= 2)
        def _():
            o_ref[0] = o_ref[0] - dot(slab[0, 0], rhs[0], 1, 1)

        for s in range(1, slots):
            o_ref[s] = o_ref[s] - dot(slab[0, s], rhs[0], 1, 1)

    @pl.when(c >= 2)
    def _():
        w1 = dot(inverse[1], dot(inverse[1], rhs[1]), 0, 0)
        w_high[1], w_low[1] = split(w1)
        w_high[0], w_low[0] = split(rhs[0] - dot(keep[1], w1, 0, 0))

    @pl.when((c >= 2) & (r < 2))
    def _():
        o_ref[0] = jnp.zeros((size, size), F32)

    def trail(which, s, pieces):
        for p in pieces:
            ensure(which, s, p)
        span = slice(pieces[0] * part_rows, (pieces[-1] + 1) * part_rows)

        @pl.when((c >= 2) & ((r >= 2) if s == 0 else (r >= 0)))
        def _():
            @pl.when(c == cols - 1)
            def _():
                for p in pieces:
                    land(which, s, p)

            base = a_ref if which == 1 else o_ref
            w = (w_high[which], w_low[which])
            o_ref[s, span] = base[s, span] - dot3(split(slab[which, s, span]), w)

    everything = tuple(range(PIECES))
    for s in range(slots):
        trail(1, s, everything)
        serve(1, 1)
    for s in range(slots - 1):
        trail(0, s, everything)
        serve(1, 1)
    for p in everything:
        trail(0, slots - 1, (p,))

    def sent(source, sem):
        pltpu.make_async_remote_copy(
            src_ref=source,
            dst_ref=source,
            send_sem=sem,
            recv_sem=tile_recv.at[0],
            device_id=(r, c),
            device_id_type=MESH,
        ).wait_send()

    for items in (FIRST + REST, BELOW, CORNER, TOP, NEXT):
        area = {}
        tile = ITEMS[items[0]][0]
        routes(items, lambda when, way, item: area.setdefault(way, (when, []))[1].append(item))
        for way, (when, sent_items) in area.items():
            height = sum(ITEMS[i][6] * ITEMS[i][7] for i in sent_items) // 8
            pl.when(when)(
                lambda tile=tile, way=way, height=height: sent(
                    tiles.at[tile, pl.ds(0, height * eighth)], tile_send.at[tile, way]
                )
            )
    for low_row, mine in ((0, r >= 2), (1, r < 2)):
        for which in range(2):

            @pl.when(mine & (c >= which) & (c < cols - 1))
            def _(low_row=low_row, which=which):
                sent(slab.at[which, pl.ds(low_row, slots - low_row)], slab_send.at[which])


def solution(mesh):
    rows, cols = mesh.shape["row"], mesh.shape["col"]
    ways = 1 + rows.bit_length() + rows // 2

    def body(choi):
        slots, size, _ = choi.shape
        half = size // 2
        vmem = pl.BlockSpec(memory_space=pltpu.VMEM)
        result = pl.pallas_call(
            functools.partial(kernel, rows, cols),
            out_shape=pltpu.VMEM(choi.shape, F32),
            in_specs=[vmem],
            out_specs=vmem,
            scratch_shapes=[
                pltpu.VMEM((5, size, size), F32),
                pltpu.VMEM((2, slots, size, size), F32),
                pltpu.VMEM((3, half, half), F32),
                pltpu.VMEM((half, half), F32),
                pltpu.VMEM((2, size, size), F32),
                pltpu.VMEM((2, size, size), F32),
                pltpu.VMEM((2, size, size), F32),
                pltpu.VMEM((2, size, size), jnp.bfloat16),
                pltpu.VMEM((2, size, size), jnp.bfloat16),
                pltpu.SemaphoreType.DMA((5, ways)),
                pltpu.SemaphoreType.DMA((len(ITEMS),)),
                pltpu.SemaphoreType.DMA((2,)),
                pltpu.SemaphoreType.DMA((2, slots, PIECES)),
            ],
            compiler_params=pltpu.CompilerParams(collective_id=0, has_side_effects=True),
        )(choi)
        tile_row = jnp.arange(slots, dtype=jnp.int32) * rows + lax.axis_index("row")
        cleared = (lax.axis_index("col") >= 2) & (tile_row[:, None, None] < 2)
        return jnp.where(cleared, 0.0, result)

    return jax.shard_map(
        body,
        mesh=mesh,
        in_specs=(P(None, "row", "col"),),
        out_specs=P(None, "row", "col"),
        check_vma=False,
    )
```

```python
import functools

import jax
import jax.numpy as jnp
from jax import lax
from jax.experimental import pallas as pl
from jax.experimental.pallas import tpu as pltpu
from jax.sharding import PartitionSpec as P

MESH = pl.DeviceIdType.MESH
HIGHEST = lax.Precision.HIGHEST
F32 = jnp.float32

PIECES = 4
ITEMS = (
    (0, 1, 0, 0, 0, 0, 2, 4, True),
    (0, 1, 0, 0, 0, 2, 2, 4, True),
    (0, 1, 0, 0, 0, 4, 2, 8, False),
    (0, 1, 0, 0, 0, 6, 2, 8, False),
    (1, 1, 1, 0, 1, 0, 2, 8, False),
    (1, 1, 1, 0, 1, 2, 2, 8, False),
    (1, 1, 1, 0, 1, 4, 2, 8, False),
    (1, 1, 1, 0, 1, 6, 2, 8, False),
    (2, 1, 1, 1, 1, 0, 4, 4, False),
    (2, 1, 1, 1, 1, 4, 2, 8, False),
    (2, 1, 1, 1, 1, 6, 2, 8, False),
    (3, 0, 0, None, 2, 0, 2, 8, False),
    (3, 0, 0, None, 2, 2, 2, 8, False),
    (3, 0, 0, None, 2, 4, 2, 8, False),
    (3, 0, 0, None, 2, 6, 2, 8, False),
    (4, 1, 1, None, 2, 0, 2, 8, False),
    (4, 1, 1, None, 2, 2, 2, 8, False),
    (4, 1, 1, None, 2, 4, 2, 8, False),
    (4, 1, 1, None, 2, 6, 2, 8, False),
)
FIRST, REST, BELOW, CORNER, TOP, NEXT = (
    (0, 1), (2, 3), (4, 5, 6, 7), (8, 9, 10), (11, 12, 13, 14), (15, 16, 17, 18),
)

TICKS = {
    "first": (3, 0, 0),
    "start": (1, 0, 0),
    0: (
        (0, 1, 1, 0, 1, 1, 0, 1, 0, 1),
        (0, 0, 0, 0, 0, 1, 0, 1, 0, 1),
        (0, 0, 0, 2, 1, 0, 1, 1, 0, 0),
    ),
    1: (
        (0, 1, 1, 0, 1, 1, 0, 1, 0, 1),
        (0, 1, 1, 0, 1, 1, 0, 1, 0, 1),
        (1, 1, 0, 1, 1, 0, 1, 1, 0, 1),
    ),
    2: (
        (1, 0, 1, 1, 0, 1, 1, 0, 0, 1),
        (1, 0, 1, 1, 0, 1, 1, 0, 0, 1),
        (0, 1, 1, 0, 1, 1, 0, 1, 0, 0),
    ),
    3: (
        (1, 0, 1, 1, 0, 1, 1, 0, 0, 1, 1, 0),
        (0, 1, 1, 0, 1, 1, 0, 1, 0, 1, 0, 1),
        (1, 1, 0, 1, 1, 0, 1, 1, 0, 2, 0, 0),
    ),
}


def dot(a, b, ca=1, cb=0, precision=HIGHEST):
    return lax.dot_general(
        a, b, (((ca,), (cb,)), ((), ())), precision=precision, preferred_element_type=F32
    )


def split(x):
    high = x.astype(jnp.bfloat16)
    return high, (x - high.astype(F32)).astype(jnp.bfloat16)


def dot3(a, b):
    (ah, al), (bh, bl) = a, b

    def one(x, y):
        return jnp.dot(x, y, preferred_element_type=F32)

    return one(al, bh) + one(ah, bl) + one(ah, bh)


def pivot_rows(rows, rest, lane, sub, first):
    n = rows.shape[1]
    wide = [jnp.broadcast_to(rows[j : j + 1, :], (8, n)) for j in range(8)]

    def spread(x):
        columns = [
            jnp.sum(jnp.where(lane == first + j, x, 0.0), axis=1, keepdims=True) for j in range(8)
        ]
        return [jnp.broadcast_to(c, (8, n)) for c in columns]

    columns = spread(rows)
    below = None if rest is None else spread(rest)
    entry = [
        [jnp.broadcast_to(columns[j][i : i + 1, :], (8, n)) if j <= i else None for j in range(8)]
        for i in range(8)
    ]
    final = jnp.zeros((8, n), F32)
    for j in range(8):
        here = lane == first + j
        pivot = entry[j][j]
        inverse = 1.0 / pivot
        base = jnp.where(here, 1.0, wide[j])
        final = jnp.where(sub == j, base * lax.rsqrt(pivot), final)
        if rest is not None:
            scale = below[j] * inverse
            rest = jnp.where(here, 0.0, rest) - scale * base
            for t in range(j + 1, 8):
                below[t] = below[t] - scale * entry[t][j]
        for i in range(j + 1, 8):
            scale = entry[i][j] * inverse
            wide[i] = jnp.where(here, 0.0, wide[i]) - scale * base
            for t in range(j + 1, i + 1):
                entry[i][t] = entry[i][t] - scale * entry[t][j]
    return final, rest


def invert_factor(z_ref, between):
    n = z_ref.shape[0]
    lane = lax.broadcasted_iota(jnp.int32, (8, n), 1)
    sub = lax.broadcasted_iota(jnp.int32, (8, n), 0)
    wide_lane = lax.broadcasted_iota(jnp.int32, (16, n), 1)
    wide_row = lax.broadcasted_iota(jnp.int32, (16, n), 0)
    all_lane = lax.broadcasted_iota(jnp.int32, (n, n), 1)
    all_row = lax.broadcasted_iota(jnp.int32, (n, n), 0)

    def panel(first):
        last = first + 16
        top, rest = pivot_rows(z_ref[first : first + 8, :], z_ref[first + 8 : last, :], lane, sub, first)
        bottom, _ = pivot_rows(rest, None, lane, sub, first + 8)
        final = jnp.concatenate([top, bottom], axis=0)
        right = jnp.where((wide_lane < last) & (wide_lane > first + wide_row), 0.0, final)
        z_ref[first:last, :] = right
        if last < n:
            left = jnp.where(wide_lane >= last, final, 0.0)
            change = dot(left, right, 0, 0)
            mine = (all_lane >= first) & (all_lane < last)
            z_ref[last:, :] = jnp.where(mine, 0.0, z_ref[...])[last:] - change[last:]

    for part in range(n // 16):
        panel(16 * part)
        between(part * 128 // n)
    z_ref[...] = jnp.where(all_lane <= all_row, z_ref[...], 0.0)


def kernel(
    rows, cols, x_ref, o_ref, a_ref, tiles, slab, blocks, work, inverse, rhs, keep, w_high, w_low,
    load, tile_send, tile_recv, slab_send, slab_recv,
):
    fill = pltpu.make_async_copy(x_ref, a_ref, load)
    fill.start()
    slots, size, _ = a_ref.shape
    half = size // 2
    eighth = size // 8
    part_rows = size // PIECES
    r = lax.axis_index("row")
    c = lax.axis_index("col")
    bits = [k for k in range(rows.bit_length()) if (1 << k) < rows][::-1]
    leaders = list(range(2, rows, 2))
    far_leaders = [q for q in leaders if q & (q - 1)]

    def across(k):
        return r + (1 << k) * (1 - 2 * ((r // (1 << k)) % 2))

    barrier = pltpu.get_barrier_semaphore()
    peers = []

    def greet(when, device, count=1):
        def signal():
            pl.semaphore_signal(barrier, inc=1, device_id=device, device_id_type=MESH)

        if when is None:
            signal()
            peers.append(1)
        else:
            pl.when(when)(signal)
            peers.append(jnp.where(when, 1, 0))

    for k in bits:
        greet(None, (across(k), c))
    greet(c > 0, (r, c - 1))
    greet(c < cols - 1, (r, c + 1))
    for q in far_leaders:
        greet(r == 1, (q + 1, c))
        greet(r == q + 1, (1, c))
    fill.wait()
    pl.semaphore_wait(barrier, functools.reduce(lambda x, y: x + y, peers))

    def node(root):
        return r if root == 0 else r + 1 - 2 * (r % 2)

    def item_copy(item, source, way, device):
        tile, _, _, _, _, row0, height, width, _ = ITEMS[item]
        span = (pl.ds(row0 * eighth, height * eighth), pl.ds(0, width * eighth))
        return pltpu.make_async_remote_copy(
            src_ref=source.at[span],
            dst_ref=tiles.at[(tile,) + span],
            send_sem=tile_send.at[lanes.get((tile, way), 0)],
            recv_sem=tile_recv.at[item],
            device_id=device,
            device_id_type=MESH,
        )

    def owns(item):
        _, _, owner_row, owner_col, first_col = ITEMS[item][:5]
        return (r == owner_row) & ((c >= first_col) if owner_col is None else (c == owner_col))

    def routes(items, visit):
        for item in items:
            tile, root, owner_row, owner_col, first_col = ITEMS[item][:5]
            straight = ITEMS[item][8]
            q = node(root)
            if owner_row != root:
                visit(owns(item), 0, item)
            if owner_col is not None:
                visit((r == root) & (c >= owner_col) & (c < cols - 1), 1, item)
            if straight:
                for n in range(len(leaders)):
                    visit((c >= first_col) & (q == 0), 2 + len(bits) + n, item)
            for n, k in enumerate(bits):
                if straight and k > 0:
                    continue
                sends = (c >= first_col) & (q % (1 << (k + 1)) == 0)
                if k == 0 and owner_row != root:
                    sends = sends & ((q != 0) | (c != owner_col))
                visit(sends, 2 + n, item)

    lanes = {}
    routes(range(len(ITEMS)), lambda when, way, item: lanes.setdefault((ITEMS[item][0], way), len(lanes)))

    def target(item, way):
        root = ITEMS[item][1]
        if way == 0:
            return (root, c)
        if way == 1:
            return (root, c + 1)
        if way < 2 + len(bits):
            return (across(bits[way - 2]), c)
        return (leaders[way - 2 - len(bits)] + root, c)

    def send(item, source, ways):
        def visit(when, way, item):
            if way in ways:
                pl.when(when)(lambda: item_copy(item, source, way, target(item, way)).start())

        routes((item,), visit)

    def depth_of(root):
        q = node(root)
        return sum((q // (1 << k)) % 2 for k in bits)

    onward = range(1, 2 + len(bits) + len(leaders))

    def launch(items):
        for item in items:
            ways = onward if ITEMS[item][1] == ITEMS[item][2] else (0,)
            pl.when(owns(item))(lambda item=item, ways=ways: send(item, a_ref.at[0], ways))

    def collect(items, low, high=99, which=True):
        for item in items:
            tile, root, _, _, first_col = ITEMS[item][:5]
            depth = depth_of(root)

            @pl.when(
                which
                & (c >= first_col)
                & jnp.logical_not(owns(item))
                & (depth >= low)
                & (depth <= high)
            )
            def _(item=item, tile=tile):
                item_copy(item, tiles.at[tile], 0, (r, c)).wait_recv()
                send(item, tiles.at[tile], onward)

    def pieces(which, s):
        spans = [(p * part_rows, part_rows) for p in range(PIECES)]
        if which == 0 and s == slots - 1:
            first, rows_left = spans.pop()
            spans += [(first, rows_left // 2), (first + rows_left // 2, rows_left // 2)]
        return range(len(spans)), spans

    def slab_copy(which, s, p, source):
        span = pl.ds(*pieces(which, s)[1][p])
        return pltpu.make_async_remote_copy(
            src_ref=source.at[s, span],
            dst_ref=slab.at[which, s, span],
            send_sem=slab_send.at[which],
            recv_sem=slab_recv.at[((1 - which) * slots + s) * PIECES + p],
            device_id=(r, c + 1),
            device_id_type=MESH,
        )

    def own_slab(which, slots_from):
        for s in range(slots_from, slots):
            for p in pieces(which, s)[0]:
                slab_copy(which, s, p, a_ref).start()

    launch(FIRST + REST)
    pl.when((c == 0) & (r >= 2))(lambda: own_slab(0, 0))
    if cols > 2:
        pl.when((c == 1) & (r >= 2))(lambda: own_slab(1, 0))

    for items in (FIRST, BELOW, CORNER, TOP, NEXT):

        @pl.when(owns(items[0]))
        def _(t=ITEMS[items[0]][0]):
            tiles[t] = a_ref[0]

    def land(which, s, p):
        slab_copy(which, s, p, slab.at[which]).wait_recv()

    def pass_on(which, s, p):
        land(which, s, p)
        slab_copy(which, s, p, slab.at[which]).start()

    def orders(first):
        return [
            (which, s, p)
            for which in (1, 0)
            for s in range(first, slots)
            for p in pieces(which, s)[0]
        ]

    queues = (orders(0), orders(1), orders(1))
    done = [0, 0, 0]
    members = (r >= 2, r == 0, r == 1)

    def serve_one(n):
        if done[n] >= len(queues[n]):
            return
        which, s, p = queues[n][done[n]]
        order = [entry for entry in queues[n] if entry[0] == 0]
        mine = members[n]
        if done[n] < len(order):
            act = pass_on if cols > 2 else land
            pl.when(mine & (c == 1))(lambda: act(*order[done[n]]))
        if cols > 3:
            pl.when(mine & (c >= 2) & (c < cols - 1))(lambda: pass_on(which, s, p))
        done[n] += 1

    def serve(*counts):
        for n, count in enumerate(counts):
            for _ in range(count):
                serve_one(n)

    def ensure(which, s, p):
        for n, queue in enumerate(queues):
            while (which, s, p) in queue and queue.index((which, s, p)) >= done[n]:
                serve_one(n)

    serve(*TICKS["first"])
    collect(FIRST, 0)
    collect(REST, 0, 0, c == 0)
    launch(BELOW)
    pl.when((c == 0) & (r == 1))(lambda: own_slab(0, 1))
    launch(CORNER)
    serve(*TICKS["start"])

    def tick(k, point):
        serve(*(counts[point] for counts in TICKS[k]))

    def between(k, point):
        part = point / 2 - 0.5
        if k == 0 and part == 0:
            collect(REST, 0, 0, (c >= 1) & (c <= 2))
            collect(BELOW + CORNER, 0, 0, c == 1)
            if cols > 2:
                pl.when((c == 1) & (r == 1))(lambda: own_slab(1, 1))
        if k == 0 and part == 1:
            collect(REST, 0, 0, c >= 3)
            collect(REST, 1, 1)
            collect(BELOW + CORNER, 0, 0, c == 2)
        if k == 0 and part == 2:
            if cols > 2:
                pl.when((c == 1) & (r == 0))(lambda: own_slab(1, 1))
            collect(REST, 2, 2)
            collect(BELOW[:2], 0, 0, c >= 3)
        if k == 0 and part == 3:
            pl.when((c == 0) & (r == 0))(lambda: own_slab(0, 1))
            collect(REST, 3)
            collect(BELOW[2:], 0, 0, c >= 3)
        if k == 1 and part == 0:
            collect(BELOW[:2], 1, 1)
        if k == 1 and part == 1:
            collect(CORNER, 0, 0, c >= 3)
            collect(BELOW[2:], 1, 1)
            launch(TOP)
        if k == 1 and part == 2:
            collect(CORNER, 1, 1)
            collect(BELOW[:2], 2, 2)
            launch(NEXT)
        if k == 1 and part == 3:
            collect(BELOW[2:] + CORNER, 2, 2)
            collect(BELOW + CORNER, 3)
        if k == 3 and part == 0:
            collect(TOP + NEXT, 1, 1)
        if k == 3 and part == 2:
            collect(TOP + NEXT, 2, 2)
        if k == 3 and part == 3:
            collect(TOP + NEXT, 3)
        tick(k, point)

    low, high = slice(0, half), slice(half, size)

    def factor(k):
        invert_factor(work, lambda part: between(k, part))

    def halfway(n):
        m = work[...]
        inverse[n, low, low] = m
        inverse[n, low, high] = jnp.zeros((half, half), F32)
        scaled = dot(blocks[1], m, 1, 1)
        blocks[0] = dot(scaled, m)
        work[...] = blocks[2] - dot(scaled, scaled, 1, 1)

    def whole(n):
        m = work[...]
        inverse[n, high, low] = -dot(m, blocks[0])
        inverse[n, high, high] = m

    work[...] = tiles[0, low, low]
    factor(0)
    tick(0, 8)
    blocks[1] = tiles[0, high, low]
    blocks[2] = tiles[0, high, high]
    halfway(0)
    tick(0, 9)
    factor(1)
    whole(0)
    tick(1, 8)

    @pl.when(c >= 1)
    def _():
        beneath = dot(tiles[1], inverse[0], 1, 1)
        keep[0] = beneath
        corner = tiles[2] - dot(beneath, beneath, 1, 1)
        work[...] = corner[low, low]
        blocks[1] = corner[high, low]
        blocks[2] = corner[high, high]
        keep[1] = dot(beneath, inverse[0])

    lower = lax.broadcasted_iota(jnp.int32, (size, size), 0) >= lax.broadcasted_iota(
        jnp.int32, (size, size), 1
    )

    @pl.when(c == 0)
    def _():
        for s in range(slots):
            o_ref[s] = dot(a_ref[s], inverse[0], 1, 1)

        @pl.when(r == 0)
        def _():
            o_ref[0] = jnp.where(lower, o_ref[0], 0.0)

    @pl.when(c >= 1)
    def _():
        tick(1, 9)
        factor(2)
        tick(2, 8)
        halfway(1)
        tick(2, 9)
        factor(3)
        pl.when(c == 1)(lambda: whole(1))

    tick(3, 8)

    @pl.when(c >= 2)
    def _():
        whole(1)
        y = dot(inverse[0], tiles[3])
        rhs[0] = tiles[4] - dot(keep[0], y)
        rhs[1] = dot(inverse[0], y, 0, 0)

    tick(3, 9)

    @pl.when(c >= 2)
    def _():
        w = dot(inverse[1], dot(inverse[1], rhs[0]), 0, 0)
        rhs[0] = w
        w_high[1], w_low[1] = split(w)

    tick(3, 10)

    @pl.when(c >= 2)
    def _():
        w_high[0], w_low[0] = split(rhs[1] - dot(keep[1], rhs[0], 0, 0))

    tick(3, 11)
    for s in range(slots):
        for p in pieces(1, s)[0]:
            ensure(1, s, p)
    for n, queue in enumerate(queues):
        while done[n] < len([entry for entry in queue if entry[0] == 0]):
            serve_one(n)

    @pl.when(c == 1)
    def _():
        rhs[0] = dot(inverse[1], keep[1])
        for s in range(slots):
            o_ref[s] = dot(a_ref[s], inverse[1], 1, 1)

        @pl.when(r == 1)
        def _():
            o_ref[0] = jnp.where(lower, o_ref[0] - dot(tiles[1], rhs[0], 1, 1), 0.0)

        @pl.when(r == 0)
        def _():
            o_ref[0] = jnp.zeros((size, size), F32)

        @pl.when(r >= 2)
        def _():
            o_ref[0] = o_ref[0] - dot(slab[0, 0], rhs[0], 1, 1)

        for s in range(1, slots):
            o_ref[s] = o_ref[s] - dot(slab[0, s], rhs[0], 1, 1)


    @pl.when((c >= 2) & (r < 2))
    def _():
        o_ref[0] = jnp.zeros((size, size), F32)

    spans = {(which, s): pieces(which, s)[1] for which in range(2) for s in range(slots)}

    def trail(which, s, ps):
        for p in ps:
            ensure(which, s, p)
        first, last = spans[which, s][ps[0]], spans[which, s][ps[-1]]
        span = slice(first[0], last[0] + last[1])

        @pl.when((c >= 2) & ((r >= 2) if s == 0 else (r >= 0)))
        def _():
            @pl.when(c == cols - 1)
            def _():
                for p in ps:
                    land(which, s, p)

            base = a_ref if which == 1 else o_ref
            w = (w_high[which], w_low[which])
            o_ref[s, span] = base[s, span] - dot3(split(slab[which, s, span]), w)

    for s in range(slots):
        trail(1, s, pieces(1, s)[0])
        serve(1, 1, 1)
    for s in range(slots - 1):
        trail(0, s, pieces(0, s)[0])
        serve(1, 1, 1)
    for p in pieces(0, slots - 1)[0]:
        trail(0, slots - 1, (p,))

    def sent(source, sem):
        pltpu.make_async_remote_copy(
            src_ref=source,
            dst_ref=source,
            send_sem=sem,
            recv_sem=tile_recv.at[0],
            device_id=(r, c),
            device_id_type=MESH,
        ).wait_send()

    for items in (FIRST + REST, BELOW, CORNER, TOP, NEXT):
        area = {}
        tile = ITEMS[items[0]][0]
        routes(items, lambda when, way, item: area.setdefault(way, (when, []))[1].append(item))
        for way, (when, sent_items) in area.items():
            height = sum(ITEMS[i][6] * ITEMS[i][7] for i in sent_items) // 8
            pl.when(when)(
                lambda tile=tile, way=way, height=height: sent(
                    tiles.at[tile, pl.ds(0, height * eighth)], tile_send.at[lanes[tile, way]]
                )
            )
    for low_row, mine in ((0, r >= 2), (1, r < 2)):
        for which in range(2):

            @pl.when(mine & (c >= which) & (c < cols - 1))
            def _(low_row=low_row, which=which):
                sent(slab.at[which, pl.ds(low_row, slots - low_row)], slab_send.at[which])


def solution(mesh):
    rows, cols = mesh.shape["row"], mesh.shape["col"]
    ways = 3 + 5 * (rows.bit_length() - 1) + rows // 2

    def body(choi):
        slots, size, _ = choi.shape
        half = size // 2
        vmem = pl.BlockSpec(memory_space=pltpu.VMEM)
        result = pl.pallas_call(
            functools.partial(kernel, rows, cols),
            out_shape=pltpu.VMEM(choi.shape, F32),
            in_specs=[pl.BlockSpec(memory_space=pl.ANY)],
            out_specs=vmem,
            scratch_shapes=[
                pltpu.VMEM(choi.shape, F32),
                pltpu.VMEM((5, size, size), F32),
                pltpu.VMEM((2, slots, size, size), F32),
                pltpu.VMEM((3, half, half), F32),
                pltpu.VMEM((half, half), F32),
                pltpu.VMEM((2, size, size), F32),
                pltpu.VMEM((2, size, size), F32),
                pltpu.VMEM((2, size, size), F32),
                pltpu.VMEM((2, size, size), jnp.bfloat16),
                pltpu.VMEM((2, size, size), jnp.bfloat16),
                pltpu.SemaphoreType.DMA,
                pltpu.SemaphoreType.DMA((ways,)),
                pltpu.SemaphoreType.DMA((len(ITEMS),)),
                pltpu.SemaphoreType.DMA((2,)),
                pltpu.SemaphoreType.DMA((2 * slots * PIECES + 1,)),
            ],
            compiler_params=pltpu.CompilerParams(collective_id=0, has_side_effects=True),
        )(choi)
        tile_row = jnp.arange(slots, dtype=jnp.int32) * rows + lax.axis_index("row")
        cleared = (lax.axis_index("col") >= 2) & (tile_row[:, None, None] < 2)
        return jnp.where(cleared, 0.0, result)

    return jax.shard_map(
        body,
        mesh=mesh,
        in_specs=(P(None, "row", "col"),),
        out_specs=P(None, "row", "col"),
        check_vma=False,
    )
```

```python
import functools

import jax
import jax.numpy as jnp
from jax import lax
from jax.experimental import pallas as pl
from jax.experimental.pallas import tpu as pltpu
from jax.sharding import PartitionSpec as P

MESH = pl.DeviceIdType.MESH
HIGHEST = lax.Precision.HIGHEST
F32 = jnp.float32

PIECES = 4
ITEMS = (
    (0, 1, 0, 0, 0, 0, 2, 4, True),
    (0, 1, 0, 0, 0, 2, 2, 4, True),
    (0, 1, 0, 0, 0, 4, 2, 8, False),
    (0, 1, 0, 0, 0, 6, 2, 8, False),
    (1, 1, 1, 0, 1, 0, 2, 8, False),
    (1, 1, 1, 0, 1, 2, 2, 8, False),
    (1, 1, 1, 0, 1, 4, 2, 8, False),
    (1, 1, 1, 0, 1, 6, 2, 8, False),
    (2, 1, 1, 1, 1, 0, 4, 4, False),
    (2, 1, 1, 1, 1, 4, 2, 8, False),
    (2, 1, 1, 1, 1, 6, 2, 8, False),
    (3, 0, 0, None, 2, 0, 2, 8, False),
    (3, 0, 0, None, 2, 2, 2, 8, False),
    (3, 0, 0, None, 2, 4, 2, 8, False),
    (3, 0, 0, None, 2, 6, 2, 8, False),
    (4, 1, 1, None, 2, 0, 2, 8, False),
    (4, 1, 1, None, 2, 2, 2, 8, False),
    (4, 1, 1, None, 2, 4, 2, 8, False),
    (4, 1, 1, None, 2, 6, 2, 8, False),
)
FIRST, REST, BELOW, CORNER, TOP, NEXT = (
    (0, 1), (2, 3), (4, 5, 6, 7), (8, 9, 10), (11, 12, 13, 14), (15, 16, 17, 18),
)

TICKS = {
    "first": (3, 0, 0),
    "start": (1, 0, 0),
    0: (
        (0, 1, 1, 0, 1, 1, 0, 1, 0, 1),
        (0, 0, 0, 0, 0, 1, 0, 1, 0, 1),
        (0, 0, 0, 2, 1, 0, 1, 1, 0, 0),
    ),
    1: (
        (0, 1, 1, 0, 1, 1, 0, 1, 0, 1),
        (0, 1, 1, 0, 1, 1, 0, 1, 0, 1),
        (1, 1, 0, 1, 1, 0, 1, 1, 0, 1),
    ),
    2: (
        (1, 0, 1, 1, 0, 1, 1, 0, 0, 1),
        (1, 0, 1, 1, 0, 1, 1, 0, 0, 1),
        (0, 1, 1, 0, 1, 1, 0, 1, 0, 0),
    ),
    3: (
        (1, 0, 1, 1, 0, 1, 1, 0, 0, 1, 1, 0),
        (0, 1, 1, 0, 1, 1, 0, 1, 0, 1, 0, 1),
        (1, 1, 0, 1, 1, 0, 1, 1, 0, 2, 0, 0),
    ),
}


def dot(a, b, ca=1, cb=0, precision=HIGHEST):
    return lax.dot_general(
        a, b, (((ca,), (cb,)), ((), ())), precision=precision, preferred_element_type=F32
    )


def split(x):
    high = x.astype(jnp.bfloat16)
    return high, (x - high.astype(F32)).astype(jnp.bfloat16)


def dot3(a, b):
    (ah, al), (bh, bl) = a, b

    def one(x, y):
        return jnp.dot(x, y, preferred_element_type=F32)

    return one(al, bh) + one(ah, bl) + one(ah, bh)


def pivot_rows(rows, rest, lane, sub, first):
    n = rows.shape[1]
    wide = [jnp.broadcast_to(rows[j : j + 1, :], (8, n)) for j in range(8)]

    def spread(x):
        columns = [
            jnp.sum(jnp.where(lane == first + j, x, 0.0), axis=1, keepdims=True) for j in range(8)
        ]
        return [jnp.broadcast_to(c, (8, n)) for c in columns]

    columns = spread(rows)
    below = None if rest is None else spread(rest)
    entry = [
        [jnp.broadcast_to(columns[j][i : i + 1, :], (8, n)) if j <= i else None for j in range(8)]
        for i in range(8)
    ]
    final = jnp.zeros((8, n), F32)
    for j in range(8):
        here = lane == first + j
        pivot = entry[j][j]
        inverse = 1.0 / pivot
        base = jnp.where(here, 1.0, wide[j])
        final = jnp.where(sub == j, base * lax.rsqrt(pivot), final)
        if rest is not None:
            scale = below[j] * inverse
            rest = jnp.where(here, 0.0, rest) - scale * base
            for t in range(j + 1, 8):
                below[t] = below[t] - scale * entry[t][j]
        for i in range(j + 1, 8):
            scale = entry[i][j] * inverse
            wide[i] = jnp.where(here, 0.0, wide[i]) - scale * base
            for t in range(j + 1, i + 1):
                entry[i][t] = entry[i][t] - scale * entry[t][j]
    return final, rest


def invert_factor(z_ref, between):
    n = z_ref.shape[0]
    lane = lax.broadcasted_iota(jnp.int32, (8, n), 1)
    sub = lax.broadcasted_iota(jnp.int32, (8, n), 0)
    wide_lane = lax.broadcasted_iota(jnp.int32, (16, n), 1)
    wide_row = lax.broadcasted_iota(jnp.int32, (16, n), 0)
    all_lane = lax.broadcasted_iota(jnp.int32, (n, n), 1)
    all_row = lax.broadcasted_iota(jnp.int32, (n, n), 0)

    def panel(first):
        last = first + 16
        top, rest = pivot_rows(z_ref[first : first + 8, :], z_ref[first + 8 : last, :], lane, sub, first)
        bottom, _ = pivot_rows(rest, None, lane, sub, first + 8)
        final = jnp.concatenate([top, bottom], axis=0)
        right = jnp.where((wide_lane < last) & (wide_lane > first + wide_row), 0.0, final)
        z_ref[first:last, :] = right
        if last < n:
            left = jnp.where(wide_lane >= last, final, 0.0)
            change = dot(left, right, 0, 0)
            mine = (all_lane >= first) & (all_lane < last)
            z_ref[last:, :] = jnp.where(mine, 0.0, z_ref[...])[last:] - change[last:]

    for part in range(n // 16):
        panel(16 * part)
        between(part * 128 // n)
    z_ref[...] = jnp.where(all_lane <= all_row, z_ref[...], 0.0)


def kernel(
    rows, cols, x_ref, o_ref, a_ref, tiles, slab, blocks, work, inverse, rhs, keep, w_high, w_low,
    load, tile_send, tile_recv, slab_send, slab_recv,
):
    fill = pltpu.make_async_copy(x_ref, a_ref, load)
    fill.start()
    slots, size, _ = a_ref.shape
    half = size // 2
    eighth = size // 8
    part_rows = size // PIECES
    r = lax.axis_index("row")
    c = lax.axis_index("col")
    bits = [k for k in range(rows.bit_length()) if (1 << k) < rows][::-1]
    leaders = list(range(2, rows, 2))
    far_leaders = [q for q in leaders if q & (q - 1)]

    def across(k):
        return r + (1 << k) * (1 - 2 * ((r // (1 << k)) % 2))

    barrier = pltpu.get_barrier_semaphore()
    peers = []

    def greet(when, device, count=1):
        def signal():
            pl.semaphore_signal(barrier, inc=1, device_id=device, device_id_type=MESH)

        if when is None:
            signal()
            peers.append(1)
        else:
            pl.when(when)(signal)
            peers.append(jnp.where(when, 1, 0))

    for k in bits:
        greet(None, (across(k), c))
    greet(c > 0, (r, c - 1))
    greet(c < cols - 1, (r, c + 1))
    for q in far_leaders:
        greet(r == 1, (q + 1, c))
        greet(r == q + 1, (1, c))
    fill.wait()
    pl.semaphore_wait(barrier, functools.reduce(lambda x, y: x + y, peers))

    def node(root):
        return r if root == 0 else r + 1 - 2 * (r % 2)

    def item_copy(item, source, way, device):
        tile, _, _, _, _, row0, height, width, _ = ITEMS[item]
        span = (pl.ds(row0 * eighth, height * eighth), pl.ds(0, width * eighth))
        return pltpu.make_async_remote_copy(
            src_ref=source.at[span],
            dst_ref=tiles.at[(tile,) + span],
            send_sem=tile_send.at[lanes.get((tile, way), 0)],
            recv_sem=tile_recv.at[item],
            device_id=device,
            device_id_type=MESH,
        )

    def owns(item):
        _, _, owner_row, owner_col, first_col = ITEMS[item][:5]
        return (r == owner_row) & ((c >= first_col) if owner_col is None else (c == owner_col))

    def routes(items, visit):
        for item in items:
            tile, root, owner_row, owner_col, first_col = ITEMS[item][:5]
            straight = ITEMS[item][8]
            q = node(root)
            if owner_row != root:
                visit(owns(item), 0, item)
            if owner_col is not None:
                visit((r == root) & (c >= owner_col) & (c < cols - 1), 1, item)
            if straight:
                for n in range(len(leaders)):
                    visit((c >= first_col) & (q == 0), 2 + len(bits) + n, item)
            for n, k in enumerate(bits):
                if straight and k > 0:
                    continue
                sends = (c >= first_col) & (q % (1 << (k + 1)) == 0)
                if k == 0 and owner_row != root:
                    sends = sends & ((q != 0) | (c != owner_col))
                visit(sends, 2 + n, item)

    lanes = {}
    routes(range(len(ITEMS)), lambda when, way, item: lanes.setdefault((ITEMS[item][0], way), len(lanes)))

    def target(item, way):
        root = ITEMS[item][1]
        if way == 0:
            return (root, c)
        if way == 1:
            return (root, c + 1)
        if way < 2 + len(bits):
            return (across(bits[way - 2]), c)
        return (leaders[way - 2 - len(bits)] + root, c)

    def send(item, source, ways):
        def visit(when, way, item):
            if way in ways:
                pl.when(when)(lambda: item_copy(item, source, way, target(item, way)).start())

        routes((item,), visit)

    def depth_of(root):
        q = node(root)
        return sum((q // (1 << k)) % 2 for k in bits)

    onward = range(1, 2 + len(bits) + len(leaders))

    def launch(items):
        for item in items:
            ways = onward if ITEMS[item][1] == ITEMS[item][2] else (0,)
            pl.when(owns(item))(lambda item=item, ways=ways: send(item, a_ref.at[0], ways))

    def collect(items, low, high=99, which=True):
        for item in items:
            tile, root, _, _, first_col = ITEMS[item][:5]
            depth = depth_of(root)

            @pl.when(
                which
                & (c >= first_col)
                & jnp.logical_not(owns(item))
                & (depth >= low)
                & (depth <= high)
            )
            def _(item=item, tile=tile):
                item_copy(item, tiles.at[tile], 0, (r, c)).wait_recv()
                send(item, tiles.at[tile], onward)

    def pieces(which, s):
        spans = [(p * part_rows, part_rows) for p in range(PIECES)]
        if which == 0 and s == slots - 1:
            first, rows_left = spans.pop()
            spans += [(first, rows_left // 2), (first + rows_left // 2, rows_left // 2)]
        return range(len(spans)), spans

    def slab_copy(which, s, p, source):
        span = pl.ds(*pieces(which, s)[1][p])
        return pltpu.make_async_remote_copy(
            src_ref=source.at[s, span],
            dst_ref=slab.at[which, s, span],
            send_sem=slab_send.at[which],
            recv_sem=slab_recv.at[((1 - which) * slots + s) * PIECES + p],
            device_id=(r, c + 1),
            device_id_type=MESH,
        )

    def own_slab(which, slots_from):
        for s in range(slots_from, slots):
            for p in pieces(which, s)[0]:
                slab_copy(which, s, p, a_ref).start()

    launch(FIRST + REST)
    pl.when((c == 0) & (r >= 2))(lambda: own_slab(0, 0))
    if cols > 2:
        pl.when((c == 1) & (r >= 2))(lambda: own_slab(1, 0))

    for items in (FIRST, BELOW, CORNER, TOP, NEXT):

        @pl.when(owns(items[0]))
        def _(t=ITEMS[items[0]][0]):
            tiles[t] = a_ref[0]

    def land(which, s, p):
        slab_copy(which, s, p, slab.at[which]).wait_recv()

    def pass_on(which, s, p):
        land(which, s, p)
        slab_copy(which, s, p, slab.at[which]).start()

    def orders(first):
        return [
            (which, s, p)
            for which in (1, 0)
            for s in range(first, slots)
            for p in pieces(which, s)[0]
        ]

    queues = (orders(0), orders(1), orders(1))
    done = [0, 0, 0]
    members = (r >= 2, r == 0, r == 1)

    def serve_one(n):
        if done[n] >= len(queues[n]):
            return
        which, s, p = queues[n][done[n]]
        order = [entry for entry in queues[n] if entry[0] == 0]
        mine = members[n]
        if done[n] < len(order):
            act = pass_on if cols > 2 else land
            pl.when(mine & (c == 1))(lambda: act(*order[done[n]]))
        if cols > 3:
            pl.when(mine & (c >= 2) & (c < cols - 1))(lambda: pass_on(which, s, p))
        done[n] += 1

    def serve(*counts):
        for n, count in enumerate(counts):
            for _ in range(count):
                serve_one(n)

    def ensure(which, s, p):
        for n, queue in enumerate(queues):
            while (which, s, p) in queue and queue.index((which, s, p)) >= done[n]:
                serve_one(n)

    serve(*TICKS["first"])
    collect(FIRST, 0)
    collect(REST, 0, 0, c == 0)
    launch(BELOW)
    pl.when((c == 0) & (r == 1))(lambda: own_slab(0, 1))
    launch(CORNER)
    serve(*TICKS["start"])

    def tick(k, point):
        serve(*(counts[point] for counts in TICKS[k]))

    def between(k, point):
        part = point / 2 - 0.5
        if k == 0 and part == 0:
            collect(REST, 0, 0, (c >= 1) & (c <= 2))
            collect(BELOW + CORNER, 0, 0, c == 1)
            if cols > 2:
                pl.when((c == 1) & (r == 1))(lambda: own_slab(1, 1))
        if k == 0 and part == 1:
            collect(REST, 0, 0, c >= 3)
            collect(REST, 1, 1)
            collect(BELOW + CORNER, 0, 0, c == 2)
        if k == 0 and part == 2:
            if cols > 2:
                pl.when((c == 1) & (r == 0))(lambda: own_slab(1, 1))
            collect(REST, 2, 2)
            collect(BELOW[:2], 0, 0, c >= 3)
        if k == 0 and part == 3:
            pl.when((c == 0) & (r == 0))(lambda: own_slab(0, 1))
            collect(REST, 3)
            collect(BELOW[2:], 0, 0, c >= 3)
        if k == 1 and part == 0:
            collect(BELOW[:2], 1, 1)
        if k == 1 and part == 1:
            collect(CORNER, 0, 0, c >= 3)
            collect(BELOW[2:], 1, 1)
            launch(TOP)
        if k == 1 and part == 2:
            collect(CORNER, 1, 1)
            collect(BELOW[:2], 2, 2)
            launch(NEXT)
        if k == 1 and part == 3:
            collect(BELOW[2:] + CORNER, 2, 2)
            collect(BELOW + CORNER, 3)
        if k == 2 and part == 1:
            collect(TOP, 1, 1)
        if k == 2 and part == 3:
            collect(TOP, 2, 2)
        if k == 3 and part == 0:
            collect(NEXT, 1, 1)
        if k == 3 and part == 1:
            collect(TOP, 3)
        if k == 3 and part == 2:
            collect(NEXT, 2, 2)
        if k == 3 and part == 3:
            collect(NEXT, 3)
        tick(k, point)

    low, high = slice(0, half), slice(half, size)

    def factor(k):
        invert_factor(work, lambda part: between(k, part))

    def halfway(n):
        m = work[...]
        inverse[n, low, low] = m
        inverse[n, low, high] = jnp.zeros((half, half), F32)
        scaled = dot(blocks[1], m, 1, 1)
        blocks[0] = dot(scaled, m)
        work[...] = blocks[2] - dot(scaled, scaled, 1, 1)

    def whole(n):
        m = work[...]
        inverse[n, high, low] = -dot(m, blocks[0])
        inverse[n, high, high] = m

    work[...] = tiles[0, low, low]
    factor(0)
    tick(0, 8)
    blocks[1] = tiles[0, high, low]
    blocks[2] = tiles[0, high, high]
    halfway(0)
    tick(0, 9)
    factor(1)
    whole(0)
    tick(1, 8)

    @pl.when(c >= 1)
    def _():
        beneath = dot(tiles[1], inverse[0], 1, 1)
        keep[0] = beneath
        corner = tiles[2] - dot(beneath, beneath, 1, 1)
        work[...] = corner[low, low]
        blocks[1] = corner[high, low]
        blocks[2] = corner[high, high]
        keep[1] = dot(beneath, inverse[0])

    lower = lax.broadcasted_iota(jnp.int32, (size, size), 0) >= lax.broadcasted_iota(
        jnp.int32, (size, size), 1
    )

    @pl.when(c == 0)
    def _():
        for s in range(slots):
            o_ref[s] = dot(a_ref[s], inverse[0], 1, 1)

        @pl.when(r == 0)
        def _():
            o_ref[0] = jnp.where(lower, o_ref[0], 0.0)

    @pl.when(c >= 1)
    def _():
        tick(1, 9)
        factor(2)
        tick(2, 8)
        halfway(1)
        tick(2, 9)
        factor(3)
        pl.when(c == 1)(lambda: whole(1))

    tick(3, 8)

    @pl.when(c >= 2)
    def _():
        whole(1)
        y = dot(inverse[0], tiles[3])
        rhs[0] = tiles[4] - dot(keep[0], y)
        rhs[1] = dot(inverse[0], y, 0, 0)

    tick(3, 9)

    @pl.when(c >= 2)
    def _():
        w = dot(inverse[1], dot(inverse[1], rhs[0]), 0, 0)
        rhs[0] = w
        w_high[1], w_low[1] = split(w)

    tick(3, 10)

    @pl.when(c >= 2)
    def _():
        w_high[0], w_low[0] = split(rhs[1] - dot(keep[1], rhs[0], 0, 0))

    tick(3, 11)
    for s in range(slots):
        for p in pieces(1, s)[0]:
            ensure(1, s, p)
    for n, queue in enumerate(queues):
        while done[n] < len([entry for entry in queue if entry[0] == 0]):
            serve_one(n)

    @pl.when(c == 1)
    def _():
        rhs[0] = dot(inverse[1], keep[1])
        for s in range(slots):
            o_ref[s] = dot(a_ref[s], inverse[1], 1, 1)

        @pl.when(r == 1)
        def _():
            o_ref[0] = jnp.where(lower, o_ref[0] - dot(tiles[1], rhs[0], 1, 1), 0.0)

        @pl.when(r == 0)
        def _():
            o_ref[0] = jnp.zeros((size, size), F32)

        @pl.when(r >= 2)
        def _():
            o_ref[0] = o_ref[0] - dot(slab[0, 0], rhs[0], 1, 1)

        for s in range(1, slots):
            o_ref[s] = o_ref[s] - dot(slab[0, s], rhs[0], 1, 1)


    @pl.when((c >= 2) & (r < 2))
    def _():
        o_ref[0] = jnp.zeros((size, size), F32)

    spans = {(which, s): pieces(which, s)[1] for which in range(2) for s in range(slots)}

    def trail(which, s, ps):
        for p in ps:
            ensure(which, s, p)
        first, last = spans[which, s][ps[0]], spans[which, s][ps[-1]]
        span = slice(first[0], last[0] + last[1])

        @pl.when((c >= 2) & ((r >= 2) if s == 0 else (r >= 0)))
        def _():
            @pl.when(c == cols - 1)
            def _():
                for p in ps:
                    land(which, s, p)

            base = a_ref if which == 1 else o_ref
            w = (w_high[which], w_low[which])
            o_ref[s, span] = base[s, span] - dot3(split(slab[which, s, span]), w)

    for s in range(slots):
        trail(1, s, pieces(1, s)[0])
        serve(1, 1, 1)
    for s in range(slots - 1):
        trail(0, s, pieces(0, s)[0])
        serve(1, 1, 1)
    for p in pieces(0, slots - 1)[0]:
        trail(0, slots - 1, (p,))

    def sent(source, sem):
        pltpu.make_async_remote_copy(
            src_ref=source,
            dst_ref=source,
            send_sem=sem,
            recv_sem=tile_recv.at[0],
            device_id=(r, c),
            device_id_type=MESH,
        ).wait_send()

    for items in (FIRST + REST, BELOW, CORNER, TOP, NEXT):
        area = {}
        tile = ITEMS[items[0]][0]
        routes(items, lambda when, way, item: area.setdefault(way, (when, []))[1].append(item))
        for way, (when, sent_items) in area.items():
            height = sum(ITEMS[i][6] * ITEMS[i][7] for i in sent_items) // 8
            pl.when(when)(
                lambda tile=tile, way=way, height=height: sent(
                    tiles.at[tile, pl.ds(0, height * eighth)], tile_send.at[lanes[tile, way]]
                )
            )
    for low_row, mine in ((0, r >= 2), (1, r < 2)):
        for which in range(2):

            @pl.when(mine & (c >= which) & (c < cols - 1))
            def _(low_row=low_row, which=which):
                sent(slab.at[which, pl.ds(low_row, slots - low_row)], slab_send.at[which])


def solution(mesh):
    rows, cols = mesh.shape["row"], mesh.shape["col"]
    ways = 3 + 5 * (rows.bit_length() - 1) + rows // 2

    def body(choi):
        slots, size, _ = choi.shape
        half = size // 2
        vmem = pl.BlockSpec(memory_space=pltpu.VMEM)
        result = pl.pallas_call(
            functools.partial(kernel, rows, cols),
            out_shape=pltpu.VMEM(choi.shape, F32),
            in_specs=[pl.BlockSpec(memory_space=pl.ANY)],
            out_specs=vmem,
            scratch_shapes=[
                pltpu.VMEM(choi.shape, F32),
                pltpu.VMEM((5, size, size), F32),
                pltpu.VMEM((2, slots, size, size), F32),
                pltpu.VMEM((3, half, half), F32),
                pltpu.VMEM((half, half), F32),
                pltpu.VMEM((2, size, size), F32),
                pltpu.VMEM((2, size, size), F32),
                pltpu.VMEM((2, size, size), F32),
                pltpu.VMEM((2, size, size), jnp.bfloat16),
                pltpu.VMEM((2, size, size), jnp.bfloat16),
                pltpu.SemaphoreType.DMA,
                pltpu.SemaphoreType.DMA((ways,)),
                pltpu.SemaphoreType.DMA((len(ITEMS),)),
                pltpu.SemaphoreType.DMA((2,)),
                pltpu.SemaphoreType.DMA((2 * slots * PIECES + 1,)),
            ],
            compiler_params=pltpu.CompilerParams(collective_id=0, has_side_effects=True),
        )(choi)
        tile_row = jnp.arange(slots, dtype=jnp.int32) * rows + lax.axis_index("row")
        cleared = (lax.axis_index("col") >= 2) & (tile_row[:, None, None] < 2)
        return jnp.where(cleared, 0.0, result)

    return jax.shard_map(
        body,
        mesh=mesh,
        in_specs=(P(None, "row", "col"),),
        out_specs=P(None, "row", "col"),
        check_vma=False,
    )
```
